256 devices in a mesh: nodes: 64 (over z, x, core), heads: 4 (over y).
Axes of the slice: x: 4, y: 4, z: 8, core: 2. Of those that a mesh axis runs over, the one named last changes fastest.
Arguments:
- nodes_in: bfloat16 [32768, 1024], P('nodes', 'heads'), may hold values from -6 to 6
- local_gain: float32 [1024], replicated, may hold values from 0.5 to 1.5
- neighbour_query_key_value: bfloat16 [3, 1024, 1024], P(None, None, 'heads'), may hold values from -0.25 to 0.25
- local_out: bfloat16 [1024, 1024], P('heads'), may hold values from -0.1875 to 0.1875
- global_gain: float32 [1024], replicated, may hold values from 0.5 to 1.5
- global_qkv: bfloat16 [3, 1024, 1024], P(None, None, 'heads'), may hold values from -0.1875 to 0.1875
- global_out: bfloat16 [1024, 1024], P('heads'), may hold values from -1.875 to 1.875
- feature_map: bfloat16 [16, 64, 128], P('heads'), may hold values from -5 to 5
- neighbour_count: int32 [256], P('nodes'), may hold values from 1 to 8
- neighbour_blocks: int32 [256, 8], P('nodes'), may hold values from 0 to 255, as said below
- metis_order: int32 [256], P('nodes'), may hold values from 0 to 255, as said below
- hashed_order: int32 [256], P('nodes'), may hold values from 0 to 255, as said below
Outputs:
- output: bfloat16 [32768, 1024], P('nodes', 'heads')
The draws below stay inside these ranges and needn't reach their ends.
Inputs may be any that keep to these rules, and one draw needn't show every extreme that they name: `neighbour_blocks`: entry 0 of block b's list is b itself; every entry lies within 2 blocks of the aligned group of 4 blocks that holds b, inside the graph; entries from neighbour_count on are unused; entries may repeat. `metis_order`: A permutation of the block ids. `hashed_order`: A permutation of the block ids. The blocks at the 4 METIS positions of aligned group g go to the aligned groups of 4 hashed positions numbered (g + k * 16) modulo 64 for k = 0 to 3, exactly 1 of them to each; which block goes to which of these groups, and to which position in it, is drawn.
All inputs are finite; a program needn't handle non-finite values.
Results may differ from the reference program's by a relative error of at most 0.015.
Values may be sent and summed in bfloat16 or wider, within the bound.
No kernel may reach another device: no remote copies, remote signals or barrier semaphores. Data moves between devices by JAX's collectives and lax.ppermute only.
A program may use at most 64 MiB of HBM per device.

```python
import jax
import jax.numpy as jnp
from jax import lax

D = 1024
HEADS = 16
HD = 64
FEAT = 128
BLOCK = 128
MAXNB = 8
HALO_BLK = 2
BLK_DEV = 4
BLOCKS = 256
NODES = 32768
N_HEADS = 4


def draw_nodes_in(key, part):
    value_rows = jax.random.normal(jax.random.fold_in(key, 43), (NODES, D), jnp.float32)
    value_rows = jnp.clip(value_rows, -6.0, 6.0)
    return value_rows.astype(jnp.bfloat16)


def draw_neighbour_query_key_value(key, part):
    weights = jax.random.normal(jax.random.fold_in(key, 53), (3, D, D), jnp.float32) * D ** (-0.5)
    weights = jnp.clip(weights, -6.0 * D ** (-0.5), 6.0 * D ** (-0.5))
    return weights.astype(jnp.bfloat16)


def block_orders(key):
    base_key = jax.random.fold_in(key, 31)
    key_metis, key_lane, key_slot = jax.random.split(base_key, 3)
    groups = BLOCKS // BLK_DEV
    lane_count = min(BLK_DEV, groups)
    stride = max(1, groups // BLK_DEV)
    metis_ids = jax.random.permutation(key_metis, BLOCKS).astype(jnp.int32)
    offsets = jnp.arange(BLK_DEV, dtype=jnp.int32)[None, :]
    lane_scores = jax.random.randint(key_lane, (groups, BLK_DEV), 0, 1 << 20) * BLK_DEV + offsets
    lane_of = jnp.argsort(lane_scores, axis=1, stable=True).astype(jnp.int32)
    slot_scores = jax.random.randint(key_slot, (groups, BLK_DEV), 0, 1 << 20) * BLK_DEV + offsets
    slot_of = jnp.argsort(slot_scores, axis=1, stable=True).astype(jnp.int32)
    group_ids = jnp.arange(groups, dtype=jnp.int32)[:, None]
    owner_group = (group_ids + lane_of % lane_count * stride) % groups
    slot_index = slot_of[owner_group, lane_of]
    position = (owner_group * BLK_DEV + slot_index).reshape(-1)
    hashed = jnp.zeros((BLOCKS,), jnp.int32).at[position].set(metis_ids)
    return (metis_ids, hashed)


def draw_metis_order(key, part):
    return block_orders(key)[0]


def draw_hashed_order(key, part):
    return block_orders(key)[1]


def draw_neighbour_blocks(key, part):
    list_key = jax.random.fold_in(key, 17)
    block_ids = jnp.arange(BLOCKS, dtype=jnp.int32)
    group_start = block_ids // BLK_DEV * BLK_DEV
    lower = jnp.maximum(group_start - HALO_BLK, 0)
    upper = jnp.minimum(group_start + BLK_DEV + HALO_BLK, BLOCKS)
    raw_draws = jax.random.randint(list_key, (BLOCKS, MAXNB - 1), 0, 1 << 20)
    picked = lower[:, None] + raw_draws % (upper - lower)[:, None]
    return jnp.concatenate([block_ids[:, None], picked.astype(jnp.int32)], axis=1)


def with_ends(values, stream_key, least, high):
    longest = values.shape.index(max(values.shape))
    spots = []
    for shift in (0, 1):
        where = [jax.random.randint(jax.random.fold_in(stream_key, axis), (), 0, length) for axis, length in enumerate(values.shape)]
        where[longest] = (where[longest] + shift) % values.shape[longest]
        spots.append(tuple(where))
    return values.at[spots[0]].set(least).at[spots[1]].set(high)


def shard_levels(stream_key, shape, pieces, smallest, top_value):
    def one(dim, parts):
        heights = jax.random.uniform(jax.random.fold_in(jax.random.fold_in(stream_key, 6), dim), (parts,), jnp.float32, smallest / len(pieces), top_value / len(pieces))
        return jnp.repeat(jnp.exp(heights), shape[dim] // parts).reshape((-1,) + (1,) * (len(shape) - dim - 1))

    loudness = one(*pieces[0])
    for cut in pieces[1:]:
        loudness = loudness * one(*cut)
    return loudness


def normal_values(key, extent, spread, limit, pieces=(), kind=jnp.bfloat16):
    factor_of = shard_levels(key, extent, pieces, -0.22, 0.18) if pieces else 1.0
    values = jax.random.normal(key, extent, jnp.float32) * spread * factor_of
    return jnp.minimum(jnp.maximum(values, -limit), limit).astype(kind)


def setup_inputs(seed: int = 0) -> dict:
    streams_of = jax.random.split(jax.random.key(seed), 13)
    nodes_in = draw_nodes_in(jax.random.fold_in(streams_of[12], 71), 0)
    local_gain = jnp.clip(1.0 + 0.1 * jax.random.normal(streams_of[1], (D,), jnp.float32), 0.5, 1.5)
    neighbour_query_key_value = draw_neighbour_query_key_value(jax.random.fold_in(streams_of[12], 71), 0)
    local_out = normal_values(streams_of[3], (D, D), D ** -0.5, 0.1875, ((0, 4),))
    global_gain = jnp.clip(1.0 + 0.1 * jax.random.normal(streams_of[4], (D,), jnp.float32), 0.5, 1.5)
    global_qkv = normal_values(streams_of[5], (3, D, D), D ** -0.5, 0.1875, ((2, 4),))
    global_out = normal_values(streams_of[6], (D, D), (10.0 * D ** -0.5), 1.875, ((0, 4),))
    feature_map = normal_values(streams_of[7], (HEADS, HD, FEAT), 1.0, 5.0, ((0, 4),))
    neighbour_count = with_ends(jax.random.randint(streams_of[8], (BLOCKS,), 1, MAXNB + 1), jax.random.fold_in(streams_of[8], 1), 1, MAXNB).astype(jnp.int32)
    neighbour_blocks = draw_neighbour_blocks(jax.random.fold_in(streams_of[12], 71), 0)
    metis_order = draw_metis_order(jax.random.fold_in(streams_of[12], 71), 0)
    hashed_order = draw_hashed_order(jax.random.fold_in(streams_of[12], 71), 0)
    return {"nodes_in": nodes_in, "local_gain": local_gain, "neighbour_query_key_value": neighbour_query_key_value, "local_out": local_out, "global_gain": global_gain, "global_qkv": global_qkv, "global_out": global_out, "feature_map": feature_map, "neighbour_count": neighbour_count, "neighbour_blocks": neighbour_blocks, "metis_order": metis_order, "hashed_order": hashed_order}


EPSILON = 1e-06

def root_scale(row_data, gain_vector):
    as_float = row_data.astype(jnp.float32)
    mean_square = lax.optimization_barrier(jnp.mean(as_float * as_float, axis=-1, keepdims=True))
    return (as_float * lax.rsqrt(mean_square + EPSILON) * gain_vector).astype(jnp.bfloat16)

def project_three(rescaled_input, triple_weight):
    return [jnp.dot(rescaled_input, triple_weight[index], preferred_element_type=jnp.float32).astype(jnp.bfloat16) for index in range(3)]

def head_groups_sum(mixed_heads, out_weight):
    group_width = D // N_HEADS
    summed = jnp.zeros((mixed_heads.shape[0], D), jnp.float32)
    for group_index in range(N_HEADS):
        lower = group_index * group_width
        part_value = jnp.dot(mixed_heads[:, lower:lower + group_width], out_weight[lower:lower + group_width], preferred_element_type=jnp.float32).astype(jnp.bfloat16)
        part_value = lax.optimization_barrier(part_value)
        summed = summed + part_value.astype(jnp.float32)
    return summed

def local_attention(queries, keys_all, values_all, counts, neighbours):
    group_size = 4 if BLK_DEV % 4 == 0 else BLK_DEV
    query_groups = queries.reshape(BLOCKS // group_size, group_size, BLOCK, HEADS, HD)
    key_blocks = keys_all.reshape(BLOCKS, BLOCK, HEADS, HD)
    value_blocks = values_all.reshape(BLOCKS, BLOCK, HEADS, HD)
    slot_of_key = jnp.arange(MAXNB * BLOCK, dtype=jnp.int32) // BLOCK

    def one_group(inputs):
        query_group, index_group, count_group = inputs
        keys_sel = key_blocks[index_group].reshape(group_size, MAXNB * BLOCK, HEADS, HD)
        values_sel = value_blocks[index_group].reshape(group_size, MAXNB * BLOCK, HEADS, HD)
        scores = jnp.einsum('gqhd,gkhd->ghqk', query_group.astype(jnp.float32), keys_sel.astype(jnp.float32)) * HD ** (-0.5)
        live = slot_of_key[None, :] < count_group[:, None]
        scores = jnp.where(live[:, None, None, :], scores, -jnp.inf)
        row_max = lax.optimization_barrier(jnp.max(scores, axis=-1, keepdims=True))
        expo = jnp.exp(scores - row_max)
        totals = lax.optimization_barrier(jnp.sum(expo, axis=-1))
        local_weights = expo.astype(jnp.bfloat16)
        mixed_heads = jnp.einsum('ghqk,gkhd->gqhd', local_weights.astype(jnp.float32), values_sel.astype(jnp.float32))
        mixed_heads = mixed_heads / jnp.transpose(totals, (0, 2, 1))[..., None]
        return mixed_heads.astype(jnp.bfloat16)
    mixed_all = lax.map(one_group, (query_groups, neighbours.reshape(BLOCKS // group_size, group_size, MAXNB), counts.reshape(BLOCKS // group_size, group_size)))
    return mixed_all.reshape(NODES, D)

def feature_maps(row_data, feature_map):
    angles = jnp.einsum('nhd,hdf->nhf', row_data.reshape(NODES, HEADS, HD).astype(jnp.float32), feature_map.astype(jnp.float32)) * HD ** (-0.5)
    return (jax.nn.elu(angles) + 1.0).astype(jnp.bfloat16)

def reference(nodes_in, local_gain, neighbour_query_key_value, local_out, global_gain, global_qkv, global_out, feature_map, neighbour_count, neighbour_blocks, metis_order, hashed_order):
    local_rescaled = root_scale(nodes_in, local_gain)
    queries, keys_all, values_all = project_three(local_rescaled, neighbour_query_key_value)
    local_mixed = local_attention(queries, keys_all, values_all, neighbour_count, neighbour_blocks)
    hidden = (nodes_in.astype(jnp.float32) + head_groups_sum(local_mixed, local_out)).astype(jnp.bfloat16)
    normed_global = root_scale(hidden, global_gain)
    global_queries, global_keys, global_values = project_three(normed_global, global_qkv)
    phi_query = feature_maps(global_queries, feature_map).astype(jnp.float32)
    phi_key = feature_maps(global_keys, feature_map).astype(jnp.float32)
    summary = jnp.einsum('nhf,nhd->hfd', phi_key, global_values.reshape(NODES, HEADS, HD).astype(jnp.float32))
    key_total = lax.optimization_barrier(jnp.sum(phi_key, axis=0))
    numerator = jnp.einsum('nhf,hfd->nhd', phi_query, summary, precision=lax.Precision.HIGHEST)
    denominator = jnp.einsum('nhf,hf->nh', phi_query, key_total, precision=lax.Precision.HIGHEST)
    global_mixed = (numerator / denominator[..., None]).astype(jnp.bfloat16).reshape(NODES, D)
    metis_out = (hidden.astype(jnp.float32) + head_groups_sum(global_mixed, global_out)).astype(jnp.bfloat16)
    position = jnp.zeros((BLOCKS,), jnp.int32).at[metis_order].set(jnp.arange(BLOCKS, dtype=jnp.int32))
    source = position[hashed_order]
    return metis_out.reshape(BLOCKS, BLOCK, D)[source].reshape(NODES, D)
```

```python
import jax
import jax.numpy as jnp
from jax import lax
from jax.experimental import pallas as pl
from jax.experimental.pallas import tpu as pltpu
from jax.sharding import Mesh, PartitionSpec as P

D = 1024
HD = 64
FEAT = 128
BLOCK = 128
HALO_BLK = 2
PEERS = 4
COLS = D // PEERS
EPSILON = 1e-06
SUM_ROWS = 144
F32 = jnp.float32
BF16 = jnp.bfloat16


def vmem():
    return pl.BlockSpec(memory_space=pltpu.VMEM)


def smem():
    return pl.BlockSpec(memory_space=pltpu.SMEM)


def shifted(value, axis, steps):
    count = lax.axis_size(axis)
    return lax.ppermute(value, axis, [(i, (i + steps) % count) for i in range(count)])


def dot(a, b):
    return jnp.dot(a, b, preferred_element_type=F32)


def dot_t(a, b):
    return lax.dot_general(a, b, (((1,), (1,)), ((), ())), preferred_element_type=F32)


def dot_rows(a, b):
    return lax.dot_general(a, b, (((0,), (0,)), ((), ())), preferred_element_type=F32)


def norm_rows(scaled, parts, gain, y):
    rows = scaled.shape[0]
    for r in range(0, rows, BLOCK):
        floats = [part[r : r + BLOCK, :].astype(F32) for part in parts]
        total = sum(jnp.sum(f * f, axis=-1, keepdims=True) for f in floats)
        inverse = lax.rsqrt(total * (1.0 / D) + EPSILON)
        for k, f in enumerate(floats):
            c = lax.rem(y + PEERS - k, PEERS)
            at = pl.multiple_of(c * COLS, COLS)
            scaled[r : r + BLOCK, pl.ds(at, COLS)] = (f * inverse * gain[c]).astype(BF16)


def qkv_kernel(y_ref, x0, x1, x2, x3, gain, w, q, low, high, scaled):
    norm_rows(scaled, (x0, x1, x2, x3), gain, y_ref[0])
    rows = scaled[...]
    half = rows.shape[0] // 2
    for t in (1, 2):
        out = dot(rows, w[t]).astype(BF16)
        low[t - 1] = out[:half]
        high[t - 1] = out[half:]
    q[...] = (dot(rows, w[0]).astype(BF16).astype(F32) * HD**-0.5).astype(BF16)


def head_masks(rows, width):
    lane = lax.broadcasted_iota(jnp.int32, (rows, width), 1)
    return [(lane // HD) == h for h in range(width // HD)]


def attention_kernel(y_ref, q, before, low, high, after, bias, w, p0, p1, p2, p3, mixed):
    keys = [part[0] for part in (before, low, high, after)]
    values = [part[1] for part in (before, low, high, after)]
    width = q.shape[1]
    heads = width // HD
    masks = head_masks(BLOCK, width)
    span = keys[0].shape[0]
    for b in range(q.shape[0] // BLOCK):
        rows = q[b * BLOCK : (b + 1) * BLOCK, :].astype(F32)
        stacked = jnp.concatenate([jnp.where(m, rows, 0.0).astype(BF16) for m in masks], axis=0)
        add = bias[b]
        scores = [
            dot_t(stacked, k) + add[:, j * span : (j + 1) * span] for j, k in enumerate(keys)
        ]
        top = jnp.max(
            jnp.maximum(jnp.maximum(scores[0], scores[1]), jnp.maximum(scores[2], scores[3])),
            axis=-1,
            keepdims=True,
        )
        expo = [jnp.exp(s - top) for s in scores]
        totals = jnp.sum((expo[0] + expo[1]) + (expo[2] + expo[3]), axis=-1, keepdims=True)
        acc = sum(dot(e.astype(BF16), v) for e, v in zip(expo, values))
        acc = acc / totals
        picked = acc[:BLOCK]
        for h in range(1, heads):
            picked = jnp.where(masks[h], acc[h * BLOCK : (h + 1) * BLOCK], picked)
        mixed[b * BLOCK : (b + 1) * BLOCK, :] = picked.astype(BF16)
    project(y_ref[0], mixed, w, (p0, p1, p2, p3))


def project(y, mixed, w, outs):
    rows = mixed[...]
    for k, out in enumerate(outs):
        at = pl.multiple_of(lax.rem(y + k, PEERS) * COLS, COLS)
        out[...] = dot(rows, w[:, pl.ds(at, COLS)]).astype(BF16).astype(out.dtype)


def spread_features(features, spread):
    spread[...] = jnp.zeros(spread.shape, spread.dtype)
    for h in range(features.shape[0]):
        spread[h * HD : (h + 1) * HD, h * FEAT : (h + 1) * FEAT] = features[h]


def feature_rows(rows, spread):
    angles = dot(rows, spread) * HD**-0.5
    return jnp.where(angles > 0, angles + 1.0, jnp.exp(jnp.minimum(angles, 0.0))).astype(BF16)


def global_kernel(y_ref, to_ref, h0, h1, h2, h3, gain, w, features, send, summary, scaled, spread):
    norm_rows(scaled, (h0, h1, h2, h3), gain, y_ref[0])
    spread_features(features, spread)
    rows = scaled[...]
    gk = dot(rows, w[1]).astype(BF16)
    gv = dot(rows, w[2]).astype(BF16)
    phi = feature_rows(gk, spread[...])
    sums = dot_rows(phi, gv)
    lane = lax.broadcasted_iota(jnp.int32, (FEAT, 2 * HD), 1)
    for pair in range(2):
        a, b = 2 * pair, 2 * pair + 1
        at = pair * 2 * HD
        left = sums[a * FEAT : (a + 1) * FEAT, at : at + 2 * HD]
        right = sums[b * FEAT : (b + 1) * FEAT, at : at + 2 * HD]
        summary[0:FEAT, at : at + 2 * HD] = jnp.where(lane < HD, left, right).astype(BF16)
    totals = jnp.sum(phi.astype(F32), axis=0, keepdims=True)
    pads = [jnp.zeros((1, FEAT), F32)] * (SUM_ROWS - FEAT - PEERS)
    tail = jnp.concatenate([totals[:, h * FEAT : (h + 1) * FEAT] for h in range(PEERS)] + pads, axis=0)
    summary[FEAT:SUM_ROWS, 0:FEAT] = tail.astype(BF16)
    summary[FEAT:SUM_ROWS, FEAT : 2 * FEAT] = jnp.zeros((SUM_ROWS - FEAT, FEAT), BF16)
    gq = dot(rows, w[0]).astype(BF16)
    for b in range(PEERS):
        to = to_ref[b]
        send[to, 0:BLOCK, :] = h0[b * BLOCK : (b + 1) * BLOCK, :]
        send[to, BLOCK : 2 * BLOCK, :] = gq[b * BLOCK : (b + 1) * BLOCK, :]


def final_kernel(y_ref, from_ref, got, sums, features, w, own, p1, p2, p3, rows, mixed, spread, table, hidden):
    spread_features(features, spread)
    total = sums[0].astype(F32)
    for j in range(1, PEERS):
        total = total + sums[j].astype(F32)
    lane = lax.broadcasted_iota(jnp.int32, (FEAT, 2 * HD), 1)
    table[...] = jnp.zeros(table.shape, table.dtype)
    for h in range(PEERS):
        at = (h // 2) * 2 * HD
        mine = (lane // HD) == (h % 2)
        part = jnp.where(mine, total[0:FEAT, at : at + 2 * HD], 0.0)
        line = total[FEAT + h : FEAT + h + 1, 0:FEAT]
        column = jnp.transpose(jnp.broadcast_to(line, (FEAT, FEAT)))
        column = jnp.where(mine, column, 0.0)
        for n, value in enumerate((part, column)):
            top = value.astype(BF16)
            table[2 * n, h * FEAT : (h + 1) * FEAT, at : at + 2 * HD] = top
            table[2 * n + 1, h * FEAT : (h + 1) * FEAT, at : at + 2 * HD] = (
                value - top.astype(F32)
            ).astype(BF16)
    for b in range(PEERS):
        source = from_ref[b]
        hidden[b * BLOCK : (b + 1) * BLOCK, :] = got[source, 0:BLOCK, :]
        rows[b * BLOCK : (b + 1) * BLOCK, :] = got[source, BLOCK : 2 * BLOCK, :]
    phi = feature_rows(rows[...], spread[...])
    numerator = dot(phi, table[0]) + dot(phi, table[1])
    denominator = dot(phi, table[2]) + dot(phi, table[3])
    mixed[...] = (numerator / denominator).astype(BF16)
    project(y_ref[0], mixed, w, (own, p1, p2, p3))
    own[...] = own[...] + hidden[...].astype(F32)


def call(kernel, outs, scratch=(), aliases=None):
    def run(*args):
        specs = [smem() if a.dtype == jnp.int32 else vmem() for a in args]
        return pl.pallas_call(
            kernel,
            in_specs=specs,
            out_specs=[vmem() for _ in outs],
            out_shape=[jax.ShapeDtypeStruct(s, d) for s, d in outs],
            scratch_shapes=[pltpu.VMEM(s, d) for s, d in scratch],
            input_output_aliases=aliases or {},
        )(*args)

    return run


def scattered(pieces):
    arrived = [shifted(p, "y", k) for k, p in enumerate(pieces[1:], 1)]
    return [pieces[0], *arrived]


def added(*parts):
    return sum(p.astype(F32) for p in parts)


def body(
    nodes_in,
    local_gain,
    qkv,
    local_out,
    global_gain,
    global_qkv,
    global_out,
    feature_map,
    counts,
    neighbours,
    metis,
    hashed,
):
    nodes_axes = ("zq", "zr", "x", "c")
    devices = lax.axis_size(nodes_axes)
    device = lax.axis_index(nodes_axes)
    rows = nodes_in.shape[0]
    blocks = counts.shape[0]
    half = rows // 2
    y = lax.axis_index("y").astype(jnp.int32).reshape(1)
    gains = (local_gain.reshape(PEERS, 1, COLS), global_gain.reshape(PEERS, 1, COLS))

    inputs = [nodes_in] + [shifted(nodes_in, "y", k) for k in range(1, PEERS)]

    ids = jnp.stack([metis, hashed])
    all_ids = lax.all_to_all(
        jnp.broadcast_to(ids, (PEERS, *ids.shape)), "zq", split_axis=0, concat_axis=0, tiled=True
    )
    order = jnp.arange(PEERS, dtype=jnp.int32)
    sends = jnp.any(all_ids[:, 1][None, :, :] == metis[:, None, None], axis=2)
    to = jnp.sum(jnp.where(sends, order[None, :], 0), axis=1)
    takes = jnp.any(all_ids[:, 0][None, :, :] == hashed[:, None, None], axis=2)
    came = jnp.sum(jnp.where(takes, order[None, :], 0), axis=1)

    window = blocks + 2 * HALO_BLK
    local_index = neighbours - (device * blocks - HALO_BLK)
    slots = jnp.arange(neighbours.shape[1], dtype=jnp.int32)
    hits = (local_index[:, :, None] == jnp.arange(window, dtype=jnp.int32)) & (
        slots[None, :, None] < counts[:, None, None]
    )
    times = jnp.sum(hits.astype(F32), axis=1)
    bias = jnp.where(times > 0, jnp.log(jnp.maximum(times, 1.0)), -1e30)
    bias = jnp.repeat(bias, BLOCK, axis=1).reshape(blocks, 1, window * BLOCK)

    pair = (2, half, COLS)
    q, low, high = call(
        qkv_kernel,
        [((rows, COLS), BF16), (pair, BF16), (pair, BF16)],
        [((rows, D), BF16)],
    )(y, *inputs, gains[0], qkv)
    up = [(i, i + 1) for i in range(devices - 1)]
    before = lax.ppermute(high, nodes_axes, up)
    after = lax.ppermute(low, nodes_axes, [(j, i) for i, j in up])

    piece = ((rows, COLS), BF16)
    pieces = call(attention_kernel, [piece] * PEERS, [piece])(
        y, q, before, low, high, after, bias, local_out
    )
    hidden = added(nodes_in, *scattered(pieces)).astype(BF16)

    full = [hidden] + [shifted(hidden, "y", k) for k in range(1, PEERS)]
    send, summary = call(
        global_kernel,
        [((PEERS, 2 * BLOCK, COLS), BF16), ((SUM_ROWS, COLS), BF16)],
        [((rows, D), BF16), ((COLS, PEERS * FEAT), BF16)],
    )(y, to, *full, gains[1], global_qkv, feature_map)

    summary = added(summary, shifted(summary, "c", 1)).astype(BF16)
    summary = added(summary, *[shifted(summary, "x", k) for k in range(1, 4)]).astype(BF16)
    summary = added(summary, shifted(summary, "zr", 1)).astype(BF16)
    send = jnp.concatenate(
        [send, jnp.broadcast_to(summary, (PEERS, *summary.shape))], axis=1
    )
    got = lax.all_to_all(send, "zq", split_axis=0, concat_axis=0, tiled=True)

    outs = call(
        final_kernel,
        [((rows, COLS), F32)] + [piece] * (PEERS - 1),
        [piece, piece, ((COLS, PEERS * FEAT), BF16), ((4, PEERS * FEAT, COLS), BF16), piece],
    )(y, came, got[:, : 2 * BLOCK], got[:, 2 * BLOCK :], feature_map, global_out)
    return added(*scattered(outs)).astype(BF16)


def solution(mesh):
    fine = Mesh(mesh.devices.reshape(4, 2, 4, 2, 4), ("zq", "zr", "x", "c", "y"))
    n = ("zq", "zr", "x", "c")
    in_specs = (
        P(n, "y"),
        P(),
        P(None, None, "y"),
        P("y", None),
        P(),
        P(None, None, "y"),
        P("y", None),
        P("y", None, None),
        P(n),
        P(n, None),
        P(n),
        P(n),
    )
    return jax.shard_map(
        body, mesh=fine, in_specs=in_specs, out_specs=P(n, "y"), check_vma=False
    )
```

```python
import jax
import jax.numpy as jnp
from jax import lax
from jax.experimental import pallas as pl
from jax.experimental.pallas import tpu as pltpu
from jax.sharding import Mesh, PartitionSpec as P

D = 1024
HD = 64
FEAT = 128
BLOCK = 128
HALO_BLK = 2
PEERS = 4
COLS = D // PEERS
EPSILON = 1e-06
SUM_ROWS = 144
F32 = jnp.float32
BF16 = jnp.bfloat16


def vmem():
    return pl.BlockSpec(memory_space=pltpu.VMEM)


def smem():
    return pl.BlockSpec(memory_space=pltpu.SMEM)


def shifted(value, axis, steps):
    count = lax.axis_size(axis)
    return lax.ppermute(value, axis, [(i, (i + steps) % count) for i in range(count)])


def flipped(value, axis, mask):
    count = lax.axis_size(axis)
    return lax.ppermute(value, axis, [(i, i ^ mask) for i in range(count)])


def dot(a, b):
    return jnp.dot(a, b, preferred_element_type=F32)


def dot_t(a, b):
    return lax.dot_general(a, b, (((1,), (1,)), ((), ())), preferred_element_type=F32)


def dot_rows(a, b):
    return lax.dot_general(a, b, (((0,), (0,)), ((), ())), preferred_element_type=F32)


def norm_rows(scaled, part, gain, y):
    for r in range(0, scaled.shape[0], BLOCK):
        places = [pl.multiple_of(lax.rem(y + PEERS - k, PEERS) * COLS, COLS) for k in range(PEERS)]
        floats = [part(k, r, at) for k, at in enumerate(places)]
        total = sum(jnp.sum(f * f, axis=-1, keepdims=True) for f in floats)
        inverse = lax.rsqrt(total * (1.0 / D) + EPSILON)
        for f, at in zip(floats, places):
            line = gain[:, pl.ds(at, COLS)]
            scaled[r : r + BLOCK, pl.ds(at, COLS)] = (f * inverse * line).astype(BF16)


def preload_kernel(c_ref, x_far, gain_far, w_far, out_far, x, gain, w, cut, sems):
    at = pl.multiple_of(c_ref[0] * (D // 2), D // 2)
    pairs = ((out_far.at[:, pl.ds(at, D // 2)], cut), (x_far, x), (gain_far, gain), (w_far, w))
    copies = [pltpu.make_async_copy(a, b, sems.at[i]) for i, (a, b) in enumerate(pairs)]
    for copy in copies:
        copy.start()
    for copy in copies:
        copy.wait()


def qkv_kernel(y_ref, x0, x1, x2, x3, gain, w, q, low, high, scaled):
    parts = (x0, x1, x2, x3)
    norm_rows(scaled, lambda k, r, at: parts[k][r : r + BLOCK, :].astype(F32), gain, y_ref[0])
    rows = scaled[...]
    half = rows.shape[0] // 2
    for t in (1, 2):
        out = dot(rows, w[t]).astype(BF16)
        low[t - 1] = out[:half]
        high[t - 1] = out[half:]
    q[...] = (dot(rows, w[0]).astype(BF16).astype(F32) * HD**-0.5).astype(BF16)


def head_masks(rows, width):
    lane = lax.broadcasted_iota(jnp.int32, (rows, width), 1)
    return [(lane // HD) == h for h in range(width // HD)]


def attention_kernel(q, before, low, high, after, bias, mixed):
    keys = [part[0] for part in (before, low, high, after)]
    values = [part[1] for part in (before, low, high, after)]
    width = q.shape[1]
    heads = width // HD
    masks = head_masks(BLOCK, width)
    span = keys[0].shape[0]
    for b in range(q.shape[0] // BLOCK):
        rows = q[b * BLOCK : (b + 1) * BLOCK, :].astype(F32)
        stacked = jnp.concatenate([jnp.where(m, rows, 0.0).astype(BF16) for m in masks], axis=0)
        add = bias[b]
        scores = [
            dot_t(stacked, k) + add[:, j * span : (j + 1) * span] for j, k in enumerate(keys)
        ]
        top = jnp.max(
            jnp.maximum(jnp.maximum(scores[0], scores[1]), jnp.maximum(scores[2], scores[3])),
            axis=-1,
            keepdims=True,
        )
        expo = [jnp.exp(s - top) for s in scores]
        totals = jnp.sum((expo[0] + expo[1]) + (expo[2] + expo[3]), axis=-1, keepdims=True)
        acc = sum(dot(e.astype(BF16), v) for e, v in zip(expo, values))
        acc = acc / totals
        picked = acc[:BLOCK]
        for h in range(1, heads):
            picked = jnp.where(masks[h], acc[h * BLOCK : (h + 1) * BLOCK], picked)
        mixed[b * BLOCK : (b + 1) * BLOCK, :] = picked.astype(BF16)


def project(y, mixed, w, outs):
    rows = mixed[...]
    for k, out in enumerate(outs):
        at = pl.multiple_of(lax.rem(y + k, PEERS) * COLS, COLS)
        out[...] = dot(rows, w[:, pl.ds(at, COLS)]).astype(BF16).astype(out.dtype)


def spread_features(features, spread):
    spread[...] = jnp.zeros(spread.shape, spread.dtype)
    for h in range(features.shape[0]):
        spread[h * HD : (h + 1) * HD, h * FEAT : (h + 1) * FEAT] = features[h]


def feature_rows(rows, spread):
    angles = dot(rows, spread) * HD**-0.5
    return jnp.where(angles > 0, angles + 1.0, jnp.exp(jnp.minimum(angles, 0.0))).astype(BF16)


def global_kernel(
    y_ref, c_ref, pick, x0, x1, x2, x3, m0, m1, m2, m3, w_own, a1, a2, a3, b1, b2, b3, gain, w, features,
    s0, s1, s2, s3, u0, u1, u2, u3, summary, local, scaled, spread, queries, hidden,
):
    c = c_ref[0]
    wide = D // 2
    for side, given in ((c, (a1, a2, a3)), (1 - c, (b1, b2, b3))):
        at = pl.multiple_of(side * wide, wide)
        out = dot(m0[...], w_own[:, pl.ds(at, wide)])
        for m, part in zip((m1, m2, m3), given):
            out = out + dot(m[...], part[...])
        local[:, pl.ds(at, wide)] = out
    parts = (x0, x1, x2, x3)

    def hidden_rows(k, r, at):
        value = parts[k][r : r + BLOCK, :].astype(F32) + local[r : r + BLOCK, pl.ds(at, COLS)]
        value = value.astype(BF16)
        if k == 0:
            hidden[r : r + BLOCK, :] = value
        return value.astype(F32)

    norm_rows(scaled, hidden_rows, gain, y_ref[0])
    spread_features(features, spread)
    rows = scaled[...]
    gk = dot(rows, w[1]).astype(BF16)
    gv = dot(rows, w[2]).astype(BF16)
    phi = feature_rows(gk, spread[...])
    sums = dot_rows(phi, gv)
    lane = lax.broadcasted_iota(jnp.int32, (FEAT, 2 * HD), 1)
    for pair in range(2):
        a, b = 2 * pair, 2 * pair + 1
        at = pair * 2 * HD
        left = sums[a * FEAT : (a + 1) * FEAT, at : at + 2 * HD]
        right = sums[b * FEAT : (b + 1) * FEAT, at : at + 2 * HD]
        summary[0:FEAT, at : at + 2 * HD] = jnp.where(lane < HD, left, right).astype(BF16)
    totals = jnp.sum(phi.astype(F32), axis=0, keepdims=True)
    pads = [jnp.zeros((1, FEAT), F32)] * (SUM_ROWS - FEAT - PEERS)
    tail = jnp.concatenate([totals[:, h * FEAT : (h + 1) * FEAT] for h in range(PEERS)] + pads, axis=0)
    summary[FEAT:SUM_ROWS, 0:FEAT] = tail.astype(BF16)
    summary[FEAT:SUM_ROWS, FEAT : 2 * FEAT] = jnp.zeros((SUM_ROWS - FEAT, FEAT), BF16)
    queries[...] = dot(rows, w[0]).astype(BF16)
    for s, (send, keep) in enumerate(((s0, u0), (s1, u1), (s2, u2), (s3, u3))):
        at = pl.multiple_of(pick[s] * BLOCK, BLOCK)
        send[...] = queries[pl.ds(at, BLOCK), :]
        keep[...] = hidden[pl.ds(at, BLOCK), :]


def final_kernel(
    y_ref, place, g0, g1, g2, g3, t0, t1, t2, t3, features, w, own, p1, p2, p3, rows, mixed, spread, table
):
    spread_features(features, spread)
    total = added(t0[...], t1[...], t2[...], t3[...])
    lane = lax.broadcasted_iota(jnp.int32, (FEAT, 2 * HD), 1)
    table[...] = jnp.zeros(table.shape, table.dtype)
    for h in range(PEERS):
        at = (h // 2) * 2 * HD
        mine = (lane // HD) == (h % 2)
        part = jnp.where(mine, total[0:FEAT, at : at + 2 * HD], 0.0)
        line = total[FEAT + h : FEAT + h + 1, 0:FEAT]
        column = jnp.transpose(jnp.broadcast_to(line, (FEAT, FEAT)))
        column = jnp.where(mine, column, 0.0)
        for n, value in enumerate((part, column)):
            top = value.astype(BF16)
            table[2 * n, h * FEAT : (h + 1) * FEAT, at : at + 2 * HD] = top
            table[2 * n + 1, h * FEAT : (h + 1) * FEAT, at : at + 2 * HD] = (
                value - top.astype(F32)
            ).astype(BF16)
    for s, got in enumerate((g0, g1, g2, g3)):
        at = pl.multiple_of(place[s] * BLOCK, BLOCK)
        rows[pl.ds(at, BLOCK), :] = got[...]
    phi = feature_rows(rows[...], spread[...])
    numerator = dot(phi, table[0]) + dot(phi, table[1])
    denominator = dot(phi, table[2]) + dot(phi, table[3])
    mixed[...] = (numerator / denominator).astype(BF16)
    project(y_ref[0], mixed, w, (own, p1, p2, p3))


def sum_kernel(place, own, p1, p2, p3, u0, u1, u2, u3, out):
    for s, keep in enumerate((u0, u1, u2, u3)):
        rows = pl.ds(pl.multiple_of(place[s] * BLOCK, BLOCK), BLOCK)
        parts = [part[rows, :].astype(F32) for part in (own, p1, p2, p3)]
        out[rows, :] = (keep[...].astype(F32) + sum(parts)).astype(BF16)


def call(kernel, outs, scratch=(), limit=24, far=()):
    def run(*args):
        specs = [smem() if a.dtype == jnp.int32 else vmem() for a in args]
        args = list(args)
        for i in far:
            specs[i] = pl.BlockSpec(memory_space=pltpu.HBM)
            args[i] = pltpu.with_memory_space_constraint(args[i], pltpu.HBM)
        return pl.pallas_call(
            kernel,
            in_specs=specs,
            out_specs=[vmem() for _ in outs],
            out_shape=[jax.ShapeDtypeStruct(s, d) for s, d in outs],
            scratch_shapes=[s if not isinstance(s, tuple) else pltpu.VMEM(*s) for s in scratch],
            compiler_params=pltpu.CompilerParams(vmem_limit_bytes=limit * 2**20),
        )(*args)

    return run


def added(*parts):
    return sum(p.astype(F32) for p in parts)


def body(
    nodes_in,
    local_gain,
    qkv,
    local_out,
    global_gain,
    global_qkv,
    global_out,
    feature_map,
    counts,
    neighbours,
    metis,
    hashed,
):
    nodes_axes = ("zq", "zr", "x", "c")
    devices = lax.axis_size(nodes_axes)
    device = lax.axis_index(nodes_axes)
    rows = nodes_in.shape[0]
    blocks = counts.shape[0]
    half = rows // 2
    y = lax.axis_index("y").astype(jnp.int32).reshape(1)
    core = lax.axis_index("c").astype(jnp.int32).reshape(1)
    gains = (local_gain.reshape(1, D), global_gain.reshape(1, D))

    inputs = [nodes_in] + [shifted(nodes_in, "y", k) for k in range(1, PEERS)]
    given = (nodes_in, gains[0], qkv, local_out)
    own_x, own_gain, qkv, mine = call(
        preload_kernel,
        [(g.shape, g.dtype) for g in given[:3]] + [((COLS, D // 2), BF16)],
        [pltpu.SemaphoreType.DMA((len(given),))],
        far=(1, 2, 3, 4),
    )(core, *given)
    ids = jnp.stack([metis, hashed])[None]
    ids = jnp.concatenate([ids, flipped(ids, "zq", 1)])
    ids = jnp.concatenate([ids, flipped(ids, "zq", 2)])
    mine = [shifted(mine, "y", k) for k in range(1, PEERS)]
    other = [shifted(m, "c", 1) for m in mine]
    order = jnp.arange(PEERS, dtype=jnp.int32)

    def where_in(wanted, lists):
        found = jnp.any(lists[:, None, :] == wanted[None, :, None], axis=2)
        return jnp.sum(jnp.where(found, order[None, :], 0), axis=1)

    pick = where_in(metis, ids[:, 1])
    place = where_in(hashed, ids[:, 0])

    window = blocks + 2 * HALO_BLK
    local_index = neighbours - (device * blocks - HALO_BLK)
    slots = jnp.arange(neighbours.shape[1], dtype=jnp.int32)
    hits = (local_index[:, :, None] == jnp.arange(window, dtype=jnp.int32)) & (
        slots[None, :, None] < counts[:, None, None]
    )
    times = jnp.sum(hits.astype(F32), axis=1)
    bias = jnp.where(times > 0, jnp.log(jnp.maximum(times, 1.0)), -1e30)
    bias = jnp.repeat(bias, BLOCK, axis=1).reshape(blocks, 1, window * BLOCK)

    pair = (2, half, COLS)
    q, low, high = call(
        qkv_kernel,
        [((rows, COLS), BF16), (pair, BF16), (pair, BF16)],
        [((rows, D), BF16)],
    )(y, own_x, *inputs[1:], own_gain, qkv)
    up = [(i, i + 1) for i in range(devices - 1)]
    before = lax.ppermute(high, nodes_axes, up)
    after = lax.ppermute(low, nodes_axes, [(j, i) for i, j in up])

    piece = ((rows, COLS), BF16)
    (mixed,) = call(attention_kernel, [piece])(q, before, low, high, after, bias)
    mixed = [mixed] + [shifted(mixed, "y", k) for k in range(1, PEERS)]

    block = ((BLOCK, COLS), BF16)
    *sends, summary = call(
        global_kernel,
        [block] * (2 * PEERS) + [((SUM_ROWS, COLS), BF16)],
        [((rows, D), F32), ((rows, D), BF16), ((COLS, PEERS * FEAT), BF16), piece, piece],
    )(y, core, pick, own_x, *inputs[1:], *mixed, local_out, *mine, *other, gains[1], global_qkv, feature_map)

    got = [sends[0]] + [flipped(sends[k], "zq", k) for k in range(1, PEERS)]
    kept = sends[PEERS:]
    kept = [kept[0]] + [flipped(kept[k], "zq", k) for k in range(1, PEERS)]
    summary = added(summary, shifted(summary, "c", 1)).astype(BF16)
    summary = added(summary, *[shifted(summary, "x", k) for k in range(1, 4)]).astype(BF16)
    summary = added(summary, shifted(summary, "zr", 1)).astype(BF16)
    parts = [summary] + [shifted(summary, "zq", k) for k in range(1, PEERS)]

    outs = call(
        final_kernel,
        [piece] * PEERS,
        [piece, piece, ((COLS, PEERS * FEAT), BF16), ((4, PEERS * FEAT, COLS), BF16)],
    )(y, place, *got, *parts, feature_map, global_out)
    outs = [outs[0]] + [shifted(p, "y", k) for k, p in enumerate(outs[1:], 1)]
    (result,) = call(sum_kernel, [piece])(place, *outs, *kept)
    return result


def solution(mesh):
    fine = Mesh(mesh.devices.reshape(4, 2, 4, 2, 4), ("zq", "zr", "x", "c", "y"))
    n = ("zq", "zr", "x", "c")
    in_specs = (
        P(n, "y"),
        P(),
        P(None, None, "y"),
        P("y", None),
        P(),
        P(None, None, "y"),
        P("y", None),
        P("y", None, None),
        P(n),
        P(n, None),
        P(n),
        P(n),
    )

    def step(*args):
        return body(*args)

    step = jax.shard_map(step, mesh=fine, in_specs=in_specs, out_specs=P(n, "y"), check_vma=False)
    return step
```

```python
import jax
import jax.numpy as jnp
from jax import lax
from jax.experimental import pallas as pl
from jax.experimental.pallas import tpu as pltpu
from jax.sharding import Mesh, PartitionSpec as P

D = 1024
HD = 64
FEAT = 128
BLOCK = 128
HALO_BLK = 2
PEERS = 4
COLS = D // PEERS
EPSILON = 1e-06
SUM_ROWS = 144
F32 = jnp.float32
BF16 = jnp.bfloat16


def vmem():
    return pl.BlockSpec(memory_space=pltpu.VMEM)


def smem():
    return pl.BlockSpec(memory_space=pltpu.SMEM)


def flipped(value, axis, mask):
    count = lax.axis_size(axis)
    return lax.ppermute(value, axis, [(i, i ^ mask) for i in range(count)])


def dot(a, b):
    return jnp.dot(a, b, preferred_element_type=F32)


def dot_t(a, b):
    return lax.dot_general(a, b, (((1,), (1,)), ((), ())), preferred_element_type=F32)


def dot_rows(a, b):
    return lax.dot_general(a, b, (((0,), (0,)), ((), ())), preferred_element_type=F32)


def norm_rows(scaled, part, gain, y):
    for r in range(0, scaled.shape[0], BLOCK):
        places = [pl.multiple_of(lax.bitwise_xor(y, k) * COLS, COLS) for k in range(PEERS)]
        floats = [part(k, r, at) for k, at in enumerate(places)]
        total = sum(jnp.sum(f * f, axis=-1, keepdims=True) for f in floats)
        inverse = lax.rsqrt(total * (1.0 / D) + EPSILON)
        for f, at in zip(floats, places):
            line = gain[:, pl.ds(at, COLS)]
            scaled[r : r + BLOCK, pl.ds(at, COLS)] = (f * inverse * line).astype(BF16)


def fetched(pairs, sems):
    copies = [pltpu.make_async_copy(a, b, sems.at[i]) for i, (a, b) in enumerate(pairs)]
    for copy in copies:
        copy.start()
    for copy in copies:
        copy.wait()


def preload_kernel(c_ref, x_far, gain_far, w_far, out_far, x, gain, w, cut, sems):
    at = pl.multiple_of(c_ref[0] * (D // 2), D // 2)
    part = out_far.at[:, pl.ds(at, D // 2)]
    fetched([(part, cut), (x_far, x), (gain_far, gain), (w_far, w)], sems)


def keys_kernel(y_ref, c_ref, x0, x1, x2, x3, gain, w, inner, outer, scaled):
    parts = (x0, x1, x2, x3)
    norm_rows(scaled, lambda k, r, at: parts[k][r : r + BLOCK, :].astype(F32), gain, y_ref[0])
    half = scaled.shape[0] // 2
    for side, out in ((1 - c_ref[0], inner), (c_ref[0], outer)):
        rows = scaled[pl.ds(pl.multiple_of(side * half, half), half), :]
        for t in (1, 2):
            out[t - 1] = dot(rows, w[t]).astype(BF16)


def head_masks(rows, width):
    lane = lax.broadcasted_iota(jnp.int32, (rows, width), 1)
    return [(lane // HD) == h for h in range(width // HD)]


def stacked_heads(rows, masks):
    rows = rows.astype(F32)
    return jnp.concatenate([jnp.where(m, rows, 0.0).astype(BF16) for m in masks], axis=0)


def picked_heads(stacked, masks):
    picked = stacked[:BLOCK]
    for h in range(1, len(masks)):
        picked = jnp.where(masks[h], stacked[h * BLOCK : (h + 1) * BLOCK], picked)
    return picked


def own_kernel(scaled, w, outer, inner, bias, q, acc, top, totals):
    q[...] = (dot(scaled[...], w[0]).astype(BF16).astype(F32) * HD**-0.5).astype(BF16)
    masks = head_masks(BLOCK, COLS)
    span = outer.shape[1]
    for b in range(q.shape[0] // BLOCK):
        rows = slice(b * BLOCK, (b + 1) * BLOCK)
        stacked = stacked_heads(q[rows, :], masks)
        add = bias[b]
        scores = [
            dot_t(stacked, part[0]) + add[:, j * span : (j + 1) * span]
            for j, part in ((1, outer), (2, inner))
        ]
        best = jnp.max(jnp.maximum(*scores), axis=-1, keepdims=True)
        expo = [jnp.exp(s - best) for s in scores]
        top[b] = jnp.broadcast_to(best, top.shape[1:])
        totals[b] = jnp.broadcast_to(jnp.sum(expo[0] + expo[1], axis=-1, keepdims=True), top.shape[1:])
        mixed = sum(dot(e.astype(BF16), part[1]) for e, part in zip(expo, (outer, inner)))
        acc[rows, :] = picked_heads(mixed, masks)


def merge_kernel(q, outer, inner, bias, acc, top, totals, mixed):
    masks = head_masks(BLOCK, COLS)
    first = masks[0][:, : 2 * HD]
    span = outer.shape[1]

    def spread_heads(rows):
        parts = [rows[h * BLOCK : (h + 1) * BLOCK] for h in range(PEERS)]
        pairs = [jnp.where(first, parts[h], parts[h + 1]) for h in (0, 2)]
        return jnp.concatenate(pairs, axis=1)

    for b in range(q.shape[0] // BLOCK):
        rows = slice(b * BLOCK, (b + 1) * BLOCK)
        stacked = stacked_heads(q[rows, :], masks)
        add = bias[b]
        scores = [
            dot_t(stacked, part[0]) + add[:, j * span : (j + 1) * span]
            for j, part in ((0, outer), (3, inner))
        ]
        seen = top[b]
        best = jnp.maximum(seen, jnp.max(jnp.maximum(*scores), axis=-1, keepdims=True))
        wide = jnp.concatenate([best, best], axis=1)
        expo = [jnp.exp(s - wide) for s in scores]
        keep = jnp.exp(seen - best)
        total = totals[b] * keep + jnp.sum(expo[0] + expo[1], axis=-1, keepdims=True)
        more = sum(dot(e.astype(BF16), part[1]) for e, part in zip(expo, (outer, inner)))
        value = acc[rows, :] * spread_heads(keep) + picked_heads(more, masks)
        mixed[rows, :] = (value / spread_heads(total)).astype(BF16)


def project(y, mixed, w, outs):
    rows = mixed[...]
    for k, out in enumerate(outs):
        at = pl.multiple_of(lax.bitwise_xor(y, k) * COLS, COLS)
        out[...] = dot(rows, w[:, pl.ds(at, COLS)]).astype(BF16).astype(out.dtype)


def spread_features(features, spread):
    spread[...] = jnp.zeros(spread.shape, spread.dtype)
    for h in range(features.shape[0]):
        spread[h * HD : (h + 1) * HD, h * FEAT : (h + 1) * FEAT] = features[h]


def feature_rows(rows, spread):
    angles = dot(rows, spread) * HD**-0.5
    return jnp.where(angles > 0, angles + 1.0, jnp.exp(jnp.minimum(angles, 0.0))).astype(BF16)


def global_kernel(
    y_ref, c_ref, x0, x1, x2, x3, m0, m1, m2, m3, w_own, a1, a2, a3, b1, b2, b3, gain, w, features,
    summary, scaled, hidden, local, spread,
):
    c = c_ref[0]
    wide = D // 2
    for side, given in ((c, (a1, a2, a3)), (1 - c, (b1, b2, b3))):
        at = pl.multiple_of(side * wide, wide)
        out = dot(m0[...], w_own[:, pl.ds(at, wide)])
        for m, part in zip((m1, m2, m3), given):
            out = out + dot(m[...], part[...])
        local[:, pl.ds(at, wide)] = out
    parts = (x0, x1, x2, x3)

    def hidden_rows(k, r, at):
        value = parts[k][r : r + BLOCK, :].astype(F32) + local[r : r + BLOCK, pl.ds(at, COLS)]
        value = value.astype(BF16)
        if k == 0:
            hidden[r : r + BLOCK, :] = value
        return value.astype(F32)

    norm_rows(scaled, hidden_rows, gain, y_ref[0])
    spread_features(features, spread)
    rows = scaled[...]
    gk = dot(rows, w[1]).astype(BF16)
    gv = dot(rows, w[2]).astype(BF16)
    phi = feature_rows(gk, spread[...])
    sums = dot_rows(phi, gv)
    lane = lax.broadcasted_iota(jnp.int32, (FEAT, 2 * HD), 1)
    totals = jnp.sum(phi.astype(F32), axis=0, keepdims=True)
    pads = [jnp.zeros((SUM_ROWS - FEAT - 2, FEAT), F32)]
    halves = []
    for pair in range(2):
        heads = (2 * pair, 2 * pair + 1)
        at = pair * 2 * HD
        left, right = (sums[h * FEAT : (h + 1) * FEAT, at : at + 2 * HD] for h in heads)
        lines = [totals[:, h * FEAT : (h + 1) * FEAT] for h in heads]
        halves.append(jnp.concatenate([jnp.where(lane < HD, left, right), *lines, *pads], axis=0))
    summary[...] = jnp.concatenate(halves, axis=1).astype(BF16)


def queries_kernel(pick, scaled, hidden, w, s0, s1, s2, s3, u0, u1, u2, u3, queries):
    queries[...] = dot(scaled[...], w[0]).astype(BF16)
    for s, (send, keep) in enumerate(((s0, u0), (s1, u1), (s2, u2), (s3, u3))):
        at = pl.multiple_of(pick[s] * BLOCK, BLOCK)
        send[...] = queries[pl.ds(at, BLOCK), :]
        keep[...] = hidden[pl.ds(at, BLOCK), :]


def final_kernel(
    y_ref, place, g0, g1, g2, g3, t0, t1, t2, t3, features, w, own, p1, p2, p3, rows, mixed, spread, table
):
    spread_features(features, spread)
    lane = lax.broadcasted_iota(jnp.int32, (FEAT, 2 * HD), 1)
    table[...] = jnp.zeros(table.shape, table.dtype)
    whole = added(t0[...], t1[...], t2[...], t3[...])
    halves = (whole[:, :FEAT], whole[:, FEAT:])
    for h in range(PEERS):
        half = halves[h // 2]
        at = (h // 2) * 2 * HD
        inside = (lane // HD) == (h % 2)
        line = half[FEAT + h % 2 : FEAT + h % 2 + 1, :]
        column = jnp.transpose(jnp.broadcast_to(line, (FEAT, FEAT)))
        for n, value in enumerate((half[0:FEAT, :], column)):
            spot = (n, slice(h * FEAT, (h + 1) * FEAT), slice(at, at + 2 * HD))
            table[spot] = jnp.where(inside, value, 0.0).astype(BF16)
    for s, got in enumerate((g0, g1, g2, g3)):
        at = pl.multiple_of(place[s] * BLOCK, BLOCK)
        rows[pl.ds(at, BLOCK), :] = got[...]
    phi = feature_rows(rows[...], spread[...])
    numerator = dot(phi, table[0])
    denominator = dot(phi, table[1])
    mixed[...] = (numerator / denominator).astype(BF16)
    project(y_ref[0], mixed, w, (own, p1, p2, p3))


def sum_kernel(place, own, p1, p2, p3, u0, u1, u2, u3, out):
    for s, keep in enumerate((u0, u1, u2, u3)):
        rows = pl.ds(pl.multiple_of(place[s] * BLOCK, BLOCK), BLOCK)
        parts = [part[rows, :].astype(F32) for part in (own, p1, p2, p3)]
        out[rows, :] = (keep[...].astype(F32) + sum(parts)).astype(BF16)


def call(kernel, outs, scratch=(), limit=24, far=()):
    def run(*args):
        specs = [smem() if a.dtype == jnp.int32 else vmem() for a in args]
        args = list(args)
        for i in far:
            specs[i] = pl.BlockSpec(memory_space=pltpu.HBM)
            args[i] = pltpu.with_memory_space_constraint(args[i], pltpu.HBM)
        return pl.pallas_call(
            kernel,
            in_specs=specs,
            out_specs=[vmem() for _ in outs],
            out_shape=[jax.ShapeDtypeStruct(s, d) for s, d in outs],
            scratch_shapes=[s if not isinstance(s, tuple) else pltpu.VMEM(*s) for s in scratch],
            compiler_params=pltpu.CompilerParams(vmem_limit_bytes=limit * 2**20),
        )(*args)

    return run


def added(*parts):
    return sum(p.astype(F32) for p in parts)


def exchanged(pieces, axis):
    got = list(pieces)
    for k in (1, 3, 2):
        got[k] = flipped(pieces[k], axis, k)
    return got


def body(
    nodes_in,
    local_gain,
    qkv,
    local_out,
    global_gain,
    global_qkv,
    global_out,
    feature_map,
    counts,
    neighbours,
    metis,
    hashed,
):
    nodes_axes = ("zq", "zr", "x", "c")
    devices = lax.axis_size(nodes_axes)
    device = lax.axis_index(nodes_axes)
    rows = nodes_in.shape[0]
    blocks = counts.shape[0]
    half = rows // 2
    y = lax.axis_index("y").astype(jnp.int32).reshape(1)
    core = lax.axis_index("c").astype(jnp.int32).reshape(1)
    gains = (local_gain.reshape(1, D), global_gain.reshape(1, D))

    piece = ((rows, COLS), BF16)
    near = exchanged([nodes_in] * PEERS, "y")
    given = (nodes_in, gains[0], qkv, local_out)
    own_x, own_gain, qkv, mine = call(
        preload_kernel,
        [(g.shape, g.dtype) for g in given[:3]] + [((COLS, D // 2), BF16)],
        [pltpu.SemaphoreType.DMA((len(given),))],
        far=(1, 2, 3, 4),
    )(core, *given)
    inputs = [own_x, *near[1:]]
    ids = jnp.stack([metis, hashed])[None]
    ids = jnp.concatenate([ids, flipped(ids, "zq", 1)])
    ids = jnp.concatenate([ids, flipped(ids, "zq", 2)])
    mine = exchanged([mine] * PEERS, "y")[1:]
    other = [flipped(m, "c", 1) for m in mine]
    order = jnp.arange(PEERS, dtype=jnp.int32)

    def where_in(wanted, lists):
        found = jnp.any(lists[:, None, :] == wanted[None, :, None], axis=2)
        return jnp.sum(jnp.where(found, order[None, :], 0), axis=1)

    pick = where_in(metis, ids[:, 1])
    place = where_in(hashed, ids[:, 0])

    window = blocks + 2 * HALO_BLK
    local_index = neighbours - (device * blocks - HALO_BLK)
    turned = (3 - local_index // HALO_BLK) * HALO_BLK + local_index % HALO_BLK
    local_index = jnp.where(core[0] == 0, local_index, turned)
    slots = jnp.arange(neighbours.shape[1], dtype=jnp.int32)
    hits = (local_index[:, :, None] == jnp.arange(window, dtype=jnp.int32)) & (
        slots[None, :, None] < counts[:, None, None]
    )
    times = jnp.sum(hits.astype(F32), axis=1)
    bias = jnp.where(times > 0, jnp.log(jnp.maximum(times, 1.0)), -1e30)
    bias = jnp.repeat(bias, BLOCK, axis=1).reshape(blocks, 1, window * BLOCK)

    pair = (2, half, COLS)
    wide = ((rows, D), BF16)
    inner, outer, scaled = call(keys_kernel, [(pair, BF16), (pair, BF16), wide])(
        y, core, own_x, *inputs[1:], own_gain, qkv
    )
    joined = [(i, i + 1) for i in range(1, devices - 1, 2)]
    joined = joined + [(j, i) for i, j in joined]
    outer_got = lax.ppermute(outer, nodes_axes, joined)
    inner_got = flipped(inner, "c", 1)
    column = ((blocks, PEERS * BLOCK, 2 * HD), F32)
    q, acc, top, totals = call(own_kernel, [piece, ((rows, COLS), F32), column, column])(
        scaled, qkv, outer, inner, bias
    )
    (mixed,) = call(merge_kernel, [piece])(q, outer_got, inner_got, bias, acc, top, totals)
    mixed = exchanged([mixed] * PEERS, "y")

    block = ((BLOCK, COLS), BF16)
    part = ((SUM_ROWS, 2 * FEAT), BF16)
    summary, scaled, hidden = call(
        global_kernel,
        [part, wide, piece],
        [((rows, D), F32), ((COLS, PEERS * FEAT), BF16)],
    )(y, core, own_x, *inputs[1:], *mixed, local_out, *mine, *other, gains[1], global_qkv, feature_map)
    sends = call(queries_kernel, [block] * (2 * PEERS), [piece])(pick, scaled, hidden, global_qkv)

    got, kept = list(sends[:PEERS]), list(sends[PEERS:])
    for k in range(1, PEERS):
        got[k] = flipped(got[k], "zq", k)
        kept[k] = flipped(kept[k], "zq", k)
    summary = added(summary, flipped(summary, "c", 1)).astype(BF16)
    summary = added(summary, flipped(summary, "zr", 1)).astype(BF16)
    summary = added(*exchanged([summary] * PEERS, "x")).astype(BF16)
    parts = exchanged([summary] * PEERS, "zq")

    outs = call(
        final_kernel,
        [piece] * PEERS,
        [piece, piece, ((COLS, PEERS * FEAT), BF16), ((2, PEERS * FEAT, COLS), BF16)],
    )(y, place, *got, *parts, feature_map, global_out)
    outs = exchanged(outs, "y")
    (result,) = call(sum_kernel, [piece])(place, *outs, *kept)
    return result


def solution(mesh):
    fine = Mesh(mesh.devices.reshape(4, 2, 4, 2, 4), ("zq", "zr", "x", "c", "y"))
    n = ("zq", "zr", "x", "c")
    in_specs = (
        P(n, "y"),
        P(),
        P(None, None, "y"),
        P("y", None),
        P(),
        P(None, None, "y"),
        P("y", None),
        P("y", None, None),
        P(n),
        P(n, None),
        P(n),
        P(n),
    )

    def step(*args):
        return body(*args)

    step = jax.shard_map(step, mesh=fine, in_specs=in_specs, out_specs=P(n, "y"), check_vma=False)

    return step
```

```python
import jax
import jax.numpy as jnp
from jax import lax
from jax.experimental import pallas as pl
from jax.experimental.pallas import tpu as pltpu
from jax.sharding import Mesh, PartitionSpec as P

D = 1024
HD = 64
FEAT = 128
BLOCK = 128
HALO_BLK = 2
PEERS = 4
COLS = D // PEERS
EPSILON = 1e-06
SUM_ROWS = 144
F32 = jnp.float32
BF16 = jnp.bfloat16


def vmem():
    return pl.BlockSpec(memory_space=pltpu.VMEM)


def smem():
    return pl.BlockSpec(memory_space=pltpu.SMEM)


def flipped(value, axis, mask):
    count = lax.axis_size(axis)
    return lax.ppermute(value, axis, [(i, i ^ mask) for i in range(count)])


def dot(a, b):
    return jnp.dot(a, b, preferred_element_type=F32)


def dot_t(a, b):
    return lax.dot_general(a, b, (((1,), (1,)), ((), ())), preferred_element_type=F32)


def dot_rows(a, b):
    return lax.dot_general(a, b, (((0,), (0,)), ((), ())), preferred_element_type=F32)


def norm_rows(scaled, part, gain, y):
    for r in range(0, scaled.shape[0], BLOCK):
        places = [pl.multiple_of(lax.bitwise_xor(y, k) * COLS, COLS) for k in range(PEERS)]
        floats = [part(k, r, at) for k, at in enumerate(places)]
        total = sum(jnp.sum(f * f, axis=-1, keepdims=True) for f in floats)
        inverse = lax.rsqrt(total * (1.0 / D) + EPSILON)
        for f, at in zip(floats, places):
            line = gain[:, pl.ds(at, COLS)]
            scaled[r : r + BLOCK, pl.ds(at, COLS)] = (f * inverse * line).astype(BF16)


def fetched(pairs, sems):
    copies = [pltpu.make_async_copy(a, b, sems.at[i]) for i, (a, b) in enumerate(pairs)]
    for copy in copies:
        copy.start()
    for copy in copies:
        copy.wait()


def preload_kernel(c_ref, x_far, gain_far, w_far, out_far, x, gain, w, cut, sems):
    at = pl.multiple_of(c_ref[0] * (D // 2), D // 2)
    part = out_far.at[:, pl.ds(at, D // 2)]
    fetched([(part, cut), (x_far, x), (gain_far, gain), (w_far, w)], sems)


def half_keys(side, scaled, w, out):
    half = scaled.shape[0] // 2
    rows = scaled[pl.ds(pl.multiple_of(side * half, half), half), :]
    for t in (1, 2):
        out[t - 1] = dot(rows, w[t]).astype(BF16)


def keys_kernel(y_ref, c_ref, x0, x1, x2, x3, gain, w, outer, scaled):
    parts = (x0, x1, x2, x3)
    norm_rows(scaled, lambda k, r, at: parts[k][r : r + BLOCK, :].astype(F32), gain, y_ref[0])
    half_keys(c_ref[0], scaled, w, outer)


def inner_kernel(c_ref, scaled, w, inner):
    half_keys(1 - c_ref[0], scaled, w, inner)


def head_masks(rows, width):
    lane = lax.broadcasted_iota(jnp.int32, (rows, width), 1)
    return [(lane // HD) == h for h in range(width // HD)]


def stacked_heads(rows, masks):
    rows = rows.astype(F32)
    return jnp.concatenate([jnp.where(m, rows, 0.0).astype(BF16) for m in masks], axis=0)


def picked_heads(stacked, masks):
    picked = stacked[:BLOCK]
    for h in range(1, len(masks)):
        picked = jnp.where(masks[h], stacked[h * BLOCK : (h + 1) * BLOCK], picked)
    return picked


def own_kernel(scaled, w, outer, inner, bias, q, acc, top, totals):
    q[...] = (dot(scaled[...], w[0]).astype(BF16).astype(F32) * HD**-0.5).astype(BF16)
    masks = head_masks(BLOCK, COLS)
    span = outer.shape[1]
    for b in range(q.shape[0] // BLOCK):
        rows = slice(b * BLOCK, (b + 1) * BLOCK)
        stacked = stacked_heads(q[rows, :], masks)
        add = bias[b]
        scores = [
            dot_t(stacked, part[0]) + add[:, j * span : (j + 1) * span]
            for j, part in ((1, outer), (2, inner))
        ]
        best = jnp.max(jnp.maximum(*scores), axis=-1, keepdims=True)
        expo = [jnp.exp(s - best) for s in scores]
        top[b] = jnp.broadcast_to(best, top.shape[1:])
        totals[b] = jnp.broadcast_to(jnp.sum(expo[0] + expo[1], axis=-1, keepdims=True), top.shape[1:])
        mixed = sum(dot(e.astype(BF16), part[1]) for e, part in zip(expo, (outer, inner)))
        acc[rows, :] = picked_heads(mixed, masks)


def merge_kernel(q, outer, inner, bias, acc, top, totals, mixed):
    masks = head_masks(BLOCK, COLS)
    first = masks[0][:, : 2 * HD]
    span = outer.shape[1]

    def spread_heads(rows):
        parts = [rows[h * BLOCK : (h + 1) * BLOCK] for h in range(PEERS)]
        pairs = [jnp.where(first, parts[h], parts[h + 1]) for h in (0, 2)]
        return jnp.concatenate(pairs, axis=1)

    for b in range(q.shape[0] // BLOCK):
        rows = slice(b * BLOCK, (b + 1) * BLOCK)
        stacked = stacked_heads(q[rows, :], masks)
        add = bias[b]
        scores = [
            dot_t(stacked, part[0]) + add[:, j * span : (j + 1) * span]
            for j, part in ((0, outer), (3, inner))
        ]
        seen = top[b]
        best = jnp.maximum(seen, jnp.max(jnp.maximum(*scores), axis=-1, keepdims=True))
        wide = jnp.concatenate([best, best], axis=1)
        expo = [jnp.exp(s - wide) for s in scores]
        keep = jnp.exp(seen - best)
        total = totals[b] * keep + jnp.sum(expo[0] + expo[1], axis=-1, keepdims=True)
        more = sum(dot(e.astype(BF16), part[1]) for e, part in zip(expo, (outer, inner)))
        value = acc[rows, :] * spread_heads(keep) + picked_heads(more, masks)
        mixed[rows, :] = (value / spread_heads(total)).astype(BF16)


def project(y, mixed, w, outs):
    rows = mixed[...]
    for k, out in enumerate(outs):
        at = pl.multiple_of(lax.bitwise_xor(y, k) * COLS, COLS)
        out[...] = dot(rows, w[:, pl.ds(at, COLS)]).astype(BF16).astype(out.dtype)


def spread_features(features, spread):
    spread[...] = jnp.zeros(spread.shape, spread.dtype)
    for h in range(features.shape[0]):
        spread[h * HD : (h + 1) * HD, h * FEAT : (h + 1) * FEAT] = features[h]


def feature_rows(rows, spread):
    angles = dot(rows, spread) * HD**-0.5
    return jnp.where(angles > 0, angles + 1.0, jnp.exp(jnp.minimum(angles, 0.0))).astype(BF16)


def global_kernel(
    y_ref, c_ref, x0, x1, x2, x3, m0, m1, m2, m3, w_own, a1, a2, a3, b1, b2, b3, gain, w, features,
    summary, scaled, hidden, local, spread,
):
    c = c_ref[0]
    wide = D // 2
    for side, given in ((c, (a1, a2, a3)), (1 - c, (b1, b2, b3))):
        at = pl.multiple_of(side * wide, wide)
        out = dot(m0[...], w_own[:, pl.ds(at, wide)])
        for m, part in zip((m1, m2, m3), given):
            out = out + dot(m[...], part[...])
        local[:, pl.ds(at, wide)] = out
    parts = (x0, x1, x2, x3)

    def hidden_rows(k, r, at):
        value = parts[k][r : r + BLOCK, :].astype(F32) + local[r : r + BLOCK, pl.ds(at, COLS)]
        value = value.astype(BF16)
        if k == 0:
            hidden[r : r + BLOCK, :] = value
        return value.astype(F32)

    norm_rows(scaled, hidden_rows, gain, y_ref[0])
    spread_features(features, spread)
    rows = scaled[...]
    gk = dot(rows, w[1]).astype(BF16)
    gv = dot(rows, w[2]).astype(BF16)
    phi = feature_rows(gk, spread[...])
    sums = dot_rows(phi, gv)
    lane = lax.broadcasted_iota(jnp.int32, (FEAT, 2 * HD), 1)
    totals = jnp.sum(phi.astype(F32), axis=0, keepdims=True)
    pads = [jnp.zeros((SUM_ROWS - FEAT - 2, FEAT), F32)]
    halves = []
    for pair in range(2):
        heads = (2 * pair, 2 * pair + 1)
        at = pair * 2 * HD
        left, right = (sums[h * FEAT : (h + 1) * FEAT, at : at + 2 * HD] for h in heads)
        lines = [totals[:, h * FEAT : (h + 1) * FEAT] for h in heads]
        halves.append(jnp.concatenate([jnp.where(lane < HD, left, right), *lines, *pads], axis=0))
    summary[...] = jnp.concatenate(halves, axis=1).astype(BF16)


def queries_kernel(pick, scaled, hidden, w, s0, s1, s2, s3, u0, u1, u2, u3, queries):
    queries[...] = dot(scaled[...], w[0]).astype(BF16)
    for s, (send, keep) in enumerate(((s0, u0), (s1, u1), (s2, u2), (s3, u3))):
        at = pl.multiple_of(pick[s] * BLOCK, BLOCK)
        send[...] = queries[pl.ds(at, BLOCK), :]
        keep[...] = hidden[pl.ds(at, BLOCK), :]


def final_kernel(
    y_ref, place, g0, g1, g2, g3, t0, t1, t2, t3, features, w, own, p1, p2, p3, rows, mixed, spread, table
):
    spread_features(features, spread)
    lane = lax.broadcasted_iota(jnp.int32, (FEAT, 2 * HD), 1)
    table[...] = jnp.zeros(table.shape, table.dtype)
    whole = added(t0[...], t1[...], t2[...], t3[...])
    halves = (whole[:, :FEAT], whole[:, FEAT:])
    for h in range(PEERS):
        half = halves[h // 2]
        at = (h // 2) * 2 * HD
        inside = (lane // HD) == (h % 2)
        line = half[FEAT + h % 2 : FEAT + h % 2 + 1, :]
        column = jnp.transpose(jnp.broadcast_to(line, (FEAT, FEAT)))
        for n, value in enumerate((half[0:FEAT, :], column)):
            spot = (n, slice(h * FEAT, (h + 1) * FEAT), slice(at, at + 2 * HD))
            table[spot] = jnp.where(inside, value, 0.0).astype(BF16)
    for s, got in enumerate((g0, g1, g2, g3)):
        at = pl.multiple_of(place[s] * BLOCK, BLOCK)
        rows[pl.ds(at, BLOCK), :] = got[...]
    phi = feature_rows(rows[...], spread[...])
    numerator = dot(phi, table[0])
    denominator = dot(phi, table[1])
    mixed[...] = (numerator / denominator).astype(BF16)
    project(y_ref[0], mixed, w, (own, p1, p2, p3))


def sum_kernel(place, own, p1, p2, p3, u0, u1, u2, u3, out):
    for s, keep in enumerate((u0, u1, u2, u3)):
        rows = pl.ds(pl.multiple_of(place[s] * BLOCK, BLOCK), BLOCK)
        parts = [part[rows, :].astype(F32) for part in (own, p1, p2, p3)]
        out[rows, :] = (keep[...].astype(F32) + sum(parts)).astype(BF16)


def call(kernel, outs, scratch=(), limit=24, far=()):
    def run(*args):
        specs = [smem() if a.dtype == jnp.int32 else vmem() for a in args]
        args = list(args)
        for i in far:
            specs[i] = pl.BlockSpec(memory_space=pltpu.HBM)
            args[i] = pltpu.with_memory_space_constraint(args[i], pltpu.HBM)
        return pl.pallas_call(
            kernel,
            in_specs=specs,
            out_specs=[vmem() for _ in outs],
            out_shape=[jax.ShapeDtypeStruct(s, d) for s, d in outs],
            scratch_shapes=[s if not isinstance(s, tuple) else pltpu.VMEM(*s) for s in scratch],
            compiler_params=pltpu.CompilerParams(vmem_limit_bytes=limit * 2**20),
        )(*args)

    return run


def added(*parts):
    return sum(p.astype(F32) for p in parts)


def exchanged(pieces, axis):
    got = list(pieces)
    for k in (1, 3, 2):
        got[k] = flipped(pieces[k], axis, k)
    return got


def body(
    nodes_in,
    local_gain,
    qkv,
    local_out,
    global_gain,
    global_qkv,
    global_out,
    feature_map,
    counts,
    neighbours,
    metis,
    hashed,
):
    nodes_axes = ("zq", "zr", "x", "c")
    devices = lax.axis_size(nodes_axes)
    device = lax.axis_index(nodes_axes)
    rows = nodes_in.shape[0]
    blocks = counts.shape[0]
    half = rows // 2
    y = lax.axis_index("y").astype(jnp.int32).reshape(1)
    core = lax.axis_index("c").astype(jnp.int32).reshape(1)
    gains = (local_gain.reshape(1, D), global_gain.reshape(1, D))

    piece = ((rows, COLS), BF16)
    near = exchanged([nodes_in] * PEERS, "y")
    given = (nodes_in, gains[0], qkv, local_out)
    own_x, own_gain, qkv, mine = call(
        preload_kernel,
        [(g.shape, g.dtype) for g in given[:3]] + [((COLS, D // 2), BF16)],
        [pltpu.SemaphoreType.DMA((len(given),))],
        far=(1, 2, 3, 4),
    )(core, *given)
    inputs = [own_x, *near[1:]]
    ids = jnp.stack([metis, hashed])[None]
    ids = jnp.concatenate([ids, flipped(ids, "zq", 1)])
    ids = jnp.concatenate([ids, flipped(ids, "zq", 2)])
    mine = exchanged([mine] * PEERS, "y")[1:]
    other = [flipped(m, "c", 1) for m in mine]
    order = jnp.arange(PEERS, dtype=jnp.int32)

    def where_in(wanted, lists):
        found = jnp.any(lists[:, None, :] == wanted[None, :, None], axis=2)
        return jnp.sum(jnp.where(found, order[None, :], 0), axis=1)

    pick = where_in(metis, ids[:, 1])
    place = where_in(hashed, ids[:, 0])

    window = blocks + 2 * HALO_BLK
    local_index = neighbours - (device * blocks - HALO_BLK)
    turned = (3 - local_index // HALO_BLK) * HALO_BLK + local_index % HALO_BLK
    local_index = jnp.where(core[0] == 0, local_index, turned)
    slots = jnp.arange(neighbours.shape[1], dtype=jnp.int32)
    hits = (local_index[:, :, None] == jnp.arange(window, dtype=jnp.int32)) & (
        slots[None, :, None] < counts[:, None, None]
    )
    times = jnp.sum(hits.astype(F32), axis=1)
    bias = jnp.where(times > 0, jnp.log(jnp.maximum(times, 1.0)), -1e30)
    bias = jnp.repeat(bias, BLOCK, axis=1).reshape(blocks, 1, window * BLOCK)

    pair = (2, half, COLS)
    wide = ((rows, D), BF16)
    outer, scaled = call(keys_kernel, [(pair, BF16), wide])(
        y, core, own_x, *inputs[1:], own_gain, qkv
    )
    joined = [(i, i + 1) for i in range(1, devices - 1, 2)]
    joined = joined + [(j, i) for i, j in joined]
    outer_got = lax.ppermute(outer, nodes_axes, joined)
    (inner,) = call(inner_kernel, [(pair, BF16)])(core, scaled, qkv)
    inner_got = flipped(inner, "c", 1)
    column = ((blocks, PEERS * BLOCK, 2 * HD), F32)
    q, acc, top, totals = call(own_kernel, [piece, ((rows, COLS), F32), column, column])(
        scaled, qkv, outer, inner, bias
    )
    (mixed,) = call(merge_kernel, [piece])(q, outer_got, inner_got, bias, acc, top, totals)
    mixed = exchanged([mixed] * PEERS, "y")

    block = ((BLOCK, COLS), BF16)
    part = ((SUM_ROWS, 2 * FEAT), BF16)
    summary, scaled, hidden = call(
        global_kernel,
        [part, wide, piece],
        [((rows, D), F32), ((COLS, PEERS * FEAT), BF16)],
    )(y, core, own_x, *inputs[1:], *mixed, local_out, *mine, *other, gains[1], global_qkv, feature_map)
    sends = call(queries_kernel, [block] * (2 * PEERS), [piece])(pick, scaled, hidden, global_qkv)

    got, kept = list(sends[:PEERS]), list(sends[PEERS:])
    for k in range(1, PEERS):
        got[k] = flipped(got[k], "zq", k)
        kept[k] = flipped(kept[k], "zq", k)
    summary = added(summary, flipped(summary, "c", 1)).astype(BF16)
    summary = added(summary, flipped(summary, "zr", 1)).astype(BF16)
    summary = added(*exchanged([summary] * PEERS, "x")).astype(BF16)
    parts = exchanged([summary] * PEERS, "zq")

    outs = call(
        final_kernel,
        [piece] * PEERS,
        [piece, piece, ((COLS, PEERS * FEAT), BF16), ((2, PEERS * FEAT, COLS), BF16)],
    )(y, place, *got, *parts, feature_map, global_out)
    outs = exchanged(outs, "y")
    (result,) = call(sum_kernel, [piece])(place, *outs, *kept)
    return result


def solution(mesh):
    fine = Mesh(mesh.devices.reshape(4, 2, 4, 2, 4), ("zq", "zr", "x", "c", "y"))
    n = ("zq", "zr", "x", "c")
    in_specs = (
        P(n, "y"),
        P(),
        P(None, None, "y"),
        P("y", None),
        P(),
        P(None, None, "y"),
        P("y", None),
        P("y", None, None),
        P(n),
        P(n, None),
        P(n),
        P(n),
    )

    def step(*args):
        return body(*args)

    step = jax.shard_map(step, mesh=fine, in_specs=in_specs, out_specs=P(n, "y"), check_vma=False)

    return step
```
